32 devices in a mesh: sector: 8 (over z, y), ops: 4 (over x, core).
Axes of the slice: x: 2, y: 2, z: 4, core: 2. Of those that a mesh axis runs over, the one named last changes fastest.
Arguments:
- wavefunction: float32 [8, 640, 640], P('sector'), may hold values from -160 to 160
- left_env: float32 [8, 16, 640, 640], P('sector', 'ops'), may hold values from -0.25 to 0.25
- right_env: float32 [8, 16, 640, 640], P('sector', 'ops'), may hold values from -0.25 to 0.25
- shift_map: int32 [4, 8], P('ops'), may hold values from 0 to 7, each once within a row
- op_counts: int32 [4, 8], P('ops', 'sector'), may hold values from 1 to 4
Outputs:
- updated_tensor: float32 [8, 640, 640], P('sector', None, 'ops')
- rotated_env: float32 [8, 16, 640, 640], P('sector', 'ops')
The draws below stay inside these ranges and needn't reach their ends.
Inputs may be any that keep to these rules, and one draw needn't show every extreme that they name: `shift_map`: each row lists every sector once.
All inputs are finite; a program needn't handle non-finite values.
Results may differ from the reference program's by a relative error of at most 0.0003.
Values sent between devices are 32-bit elements; how exact they have to be, the bound alone decides.
A program may use at most 128 MiB of HBM per device.

```python
import math
import jax
import jax.numpy as jnp
from jax import lax

MS = 640
OPS_DEV = 4
POLAR = 5
NSEC = 8
GROUPS = 4
OPS = 16


def draw_wavefunction(key, part):
    key_base = jax.random.fold_in(key, 11)
    sector_level = jnp.arange(NSEC, dtype=jnp.float32) / float(NSEC - 1)
    base_draw = jnp.clip(jax.random.normal(key_base, (NSEC, MS, MS), jnp.float32), -6.0, 6.0)
    sector_scale = 3.0 ** sector_level
    return base_draw * sector_scale[:, None, None]


def touch_ends(entries, rng, smallest, high):
    spot = [jax.random.randint(jax.random.fold_in(rng, axis), (), 0, length) for axis, length in enumerate(entries.shape)]
    main_axis = entries.shape.index(max(entries.shape))
    next_to = spot[:main_axis] + [(spot[main_axis] + 1) % entries.shape[main_axis]] + spot[main_axis + 1:]
    return entries.at[tuple(spot)].set(smallest).at[tuple(next_to)].set(high)


def levels(stream_key, extent, cuts, least, top_value):
    level = 1.0
    for dim, shards_of in cuts:
        heights = jax.random.uniform(jax.random.fold_in(jax.random.fold_in(stream_key, 6), dim), (shards_of,), jnp.float32, least / len(cuts), top_value / len(cuts))
        level = level * jnp.repeat(jnp.exp(heights), extent[dim] // shards_of).reshape((-1,) + (1,) * (len(extent) - 1 - dim))
    return level


def scatter_about(rng, dims, deviation, limit, cuts=(), kind=jnp.bfloat16):
    result = deviation * jax.random.normal(rng, dims, jnp.float32)
    if cuts:
        result = result * levels(rng, dims, cuts, -0.22, 0.18)
    return jnp.clip(result, -limit, limit).astype(kind)


def setup_inputs(seed: int = 0) -> dict:
    seeds = jax.random.split(jax.random.key(seed), 6)
    wavefunction = draw_wavefunction(jax.random.fold_in(seeds[5], 71), 0)
    left_env = scatter_about(seeds[1], (NSEC, OPS, MS, MS), MS ** -0.5, 0.25, ((0, 8), (1, 4)), jnp.float32)
    right_env = scatter_about(seeds[2], (NSEC, OPS, MS, MS), MS ** -0.5, 0.25, ((0, 8), (1, 4)), jnp.float32)
    shift_map = jax.vmap(lambda own: jax.random.permutation(own, NSEC))(jax.random.split(seeds[3], GROUPS)).reshape((GROUPS, NSEC)).astype(jnp.int32)
    op_counts = touch_ends(jax.random.randint(seeds[4], (GROUPS, NSEC), 1, OPS_DEV + 1), jax.random.fold_in(seeds[4], 1), 1, OPS_DEV).astype(jnp.int32)
    return {"wavefunction": wavefunction, "left_env": left_env, "right_env": right_env, "shift_map": shift_map, "op_counts": op_counts}


precise = lax.Precision.HIGHEST

def reference(wavefunction, left_env, right_env, shift_map, op_counts):
    sector_ids = jnp.arange(NSEC, dtype=jnp.int32)
    slots = jnp.arange(OPS, dtype=jnp.int32) % OPS_DEV

    def sector_sigma(sector_id):
        sources = shift_map[:, sector_id]
        blocks = jnp.repeat(wavefunction[sources], OPS_DEV, axis=0)
        limits = jnp.repeat(op_counts[:, sector_id], OPS_DEV, axis=0)
        active = (slots < limits).astype(jnp.float32)
        left_psi = jnp.einsum('wab,wbc->wac', left_env[sector_id], blocks, precision=precise)
        op_terms = jnp.einsum('wac,wcd->wad', left_psi, right_env[sector_id], precision=precise)
        return jnp.einsum('w,wad->ad', active, op_terms, precision=precise)
    sigma = lax.map(sector_sigma, sector_ids)
    mean_sq = lax.optimization_barrier(jnp.sum(sigma * sigma, axis=(1, 2))) / float(MS * MS)
    factor = lax.rsqrt(MS * mean_sq + 1e-06) / 2.2
    iterate = sigma * factor[:, None, None]
    for repeat_index in range(POLAR):
        gram_matrix = jnp.einsum('sab,scb->sac', iterate, iterate, precision=precise)
        iterate = 1.5 * iterate - 0.5 * jnp.einsum('sac,scb->sab', gram_matrix, iterate, precision=precise)
    updated = iterate * math.sqrt(MS)

    def rotate(sector_id):
        sources = shift_map[:, sector_id]
        rights = jnp.repeat(updated[sources], OPS_DEV, axis=0)
        half_rotated = jnp.einsum('ba,wbc->wac', updated[sector_id], left_env[sector_id], precision=precise)
        return jnp.einsum('wac,wcd->wad', half_rotated, rights, precision=precise)
    rotated = lax.map(rotate, sector_ids)
    return (updated, rotated)
```

```python
import math

import jax
import jax.numpy as jnp
from jax import lax
from jax.sharding import PartitionSpec as P

POLAR = 5
LANES, SUBLANES = 128, 8

precise = lax.Precision.HIGH


def dot(a, b):
    return jnp.dot(a, b, precision=precise, preferred_element_type=jnp.float32)


def to_tiles(block, padded):
    rows, cols = block.shape
    tiles = block.reshape(rows // SUBLANES, SUBLANES, cols // LANES, LANES)
    tiles = tiles.transpose(0, 2, 1, 3).reshape(rows * cols // (SUBLANES * LANES), SUBLANES, LANES)
    return jnp.pad(tiles, ((0, padded - tiles.shape[0]), (0, 0), (0, 0)))


def from_tiles(tiles, rows, cols):
    tiles = tiles[: rows * cols // (SUBLANES * LANES)]
    tiles = tiles.reshape(rows // SUBLANES, cols // LANES, SUBLANES, LANES)
    return tiles.transpose(0, 2, 1, 3).reshape(rows, cols)


def swap(value, axis, bit):
    size = lax.axis_size(axis)
    return lax.ppermute(value, axis, [(i, i ^ bit) for i in range(size)])


def sum_scatter(tiles, axis):
    size, here = lax.axis_size(axis), lax.axis_index(axis)
    rest = tiles.reshape((size, tiles.shape[0] // size) + tiles.shape[1:])
    bit = 1
    while bit < size:
        mine = (here // bit) % 2
        pairs = rest.reshape((rest.shape[0] // 2, 2) + rest.shape[1:])
        keep = lax.dynamic_index_in_dim(pairs, mine, 1, keepdims=False)
        give = lax.dynamic_index_in_dim(pairs, 1 - mine, 1, keepdims=False)
        rest = keep + swap(give, axis, bit)
        bit *= 2
    return rest[0]


def gather_whole(quarter, axis):
    size, here = lax.axis_size(axis), lax.axis_index(axis)
    held = quarter[None]
    bit = size // 2
    while bit:
        mine = (here // bit) % 2
        other = swap(held, axis, bit)
        first = jnp.where(mine == 0, held, other)
        second = jnp.where(mine == 0, other, held)
        held = jnp.stack([first, second], axis=1).reshape((-1,) + quarter.shape)
        bit //= 2
    return held.reshape((-1,) + quarter.shape[1:])


def polar(sigma_block):
    states = sigma_block.shape[0]
    mean_sq = jnp.sum(sigma_block * sigma_block) / float(states * states)
    iterate = sigma_block * (lax.rsqrt(states * mean_sq + 1e-06) / 2.2)

    def step(_, iterate):
        gram_matrix = jnp.einsum("ab,cb->ac", iterate, iterate, precision=precise)
        return 1.5 * iterate - 0.5 * dot(gram_matrix, iterate)

    return lax.fori_loop(0, POLAR, step, iterate) * math.sqrt(states)


def shards(wavefunction, left_env, right_env, shift_map, op_counts):
    sector_count = lax.axis_size("sector")
    group_size = lax.axis_size("ops")
    group_here = lax.axis_index("ops")
    states = wavefunction.shape[1]
    ops_here = left_env.shape[1]
    parts = sector_count * group_size
    piece = -(-states * states // (SUBLANES * LANES * parts))
    padded = piece * parts
    quarter = piece * sector_count

    whole_map = lax.all_gather(shift_map[0], "ops").reshape(parts)

    def fetch_from_quarter(own_quarter):
        pieces = own_quarter.reshape(sector_count, piece, SUBLANES, LANES)
        spread = lax.all_to_all(pieces, "sector", split_axis=0, concat_axis=0, tiled=True)
        picked = jnp.take(spread, whole_map, axis=0)
        landed = lax.all_to_all(picked, ("ops", "sector"), split_axis=0, concat_axis=0, tiled=True)
        return from_tiles(landed.reshape(padded, SUBLANES, LANES), states, states)

    psi_tiles = to_tiles(wavefunction[0], padded)
    psi_quarter = lax.dynamic_slice_in_dim(psi_tiles, group_here * quarter, quarter, 0)
    moved_block = fetch_from_quarter(psi_quarter)

    left, right = left_env[0], right_env[0]
    count = op_counts[0, 0]
    active = (jnp.arange(ops_here) < count).astype(jnp.float32)
    left_psi = jnp.einsum("wab,bc->wac", left, moved_block, precision=precise) * active[:, None, None]
    partial_sigma = jnp.einsum("wac,wcd->ad", left_psi, right, precision=precise)

    sigma_quarter = sum_scatter(to_tiles(partial_sigma, padded), "ops")
    source_sigma = fetch_from_quarter(sigma_quarter)
    sigma_block = from_tiles(gather_whole(sigma_quarter, "ops"), states, states)

    whole_tensor = polar(sigma_block)
    column_width = states // group_size
    own_columns = lax.dynamic_slice_in_dim(whole_tensor, group_here * column_width, column_width, 1)
    half_rotated = jnp.einsum("ba,wbc->wac", whole_tensor, left, precision=precise)
    source_tensor = polar(source_sigma)
    rotated = jnp.einsum("wac,cd->wad", half_rotated, source_tensor, precision=precise)
    return (own_columns[None], rotated[None])


def solution(mesh):
    return jax.shard_map(
        shards,
        mesh=mesh,
        in_specs=(
            P("sector", None, None),
            P("sector", "ops", None, None),
            P("sector", "ops", None, None),
            P("ops", None),
            P("ops", "sector"),
        ),
        out_specs=(P("sector", None, "ops"), P("sector", "ops", None, None)),
        check_vma=False,
    )
```

```python
import math

import jax
import jax.numpy as jnp
from jax import lax
from jax.sharding import PartitionSpec as P

POLAR = 5
LANES, SUBLANES = 128, 8

precise = lax.Precision.HIGH


def dot(a, b):
    return jnp.dot(a, b, precision=precise, preferred_element_type=jnp.float32)


def split(x):
    high = lax.reduce_precision(x, exponent_bits=8, mantissa_bits=7)
    return high.astype(jnp.bfloat16), (x - high).astype(jnp.bfloat16)


def stack_left(x, axis):
    high, low = split(x)
    return jnp.concatenate([high, high, low], axis=axis)


def stack_right(x, axis):
    high, low = split(x)
    return jnp.concatenate([high, low, high], axis=axis)


def to_tiles(block, padded):
    rows, cols = block.shape
    tiles = block.reshape(rows // SUBLANES, SUBLANES, cols // LANES, LANES)
    tiles = tiles.transpose(0, 2, 1, 3).reshape(rows * cols // (SUBLANES * LANES), SUBLANES, LANES)
    return jnp.pad(tiles, ((0, padded - tiles.shape[0]), (0, 0), (0, 0)))


def from_tiles(tiles, rows, cols):
    tiles = tiles[: rows * cols // (SUBLANES * LANES)]
    tiles = tiles.reshape(rows // SUBLANES, cols // LANES, SUBLANES, LANES)
    return tiles.transpose(0, 2, 1, 3).reshape(rows, cols)


def swap(value, axis, bit):
    size = lax.axis_size(axis)
    return lax.ppermute(value, axis, [(i, i ^ bit) for i in range(size)])


def sum_scatter(tiles, axis):
    size, here = lax.axis_size(axis), lax.axis_index(axis)
    rest = tiles.reshape((size, tiles.shape[0] // size) + tiles.shape[1:])
    bit = 1
    while bit < size:
        mine = (here // bit) % 2
        pairs = rest.reshape((rest.shape[0] // 2, 2) + rest.shape[1:])
        keep = lax.dynamic_index_in_dim(pairs, mine, 1, keepdims=False)
        give = lax.dynamic_index_in_dim(pairs, 1 - mine, 1, keepdims=False)
        rest = keep + swap(give, axis, bit)
        bit *= 2
    return rest[0]


def gather_whole(quarter, axis):
    size, here = lax.axis_size(axis), lax.axis_index(axis)
    held = quarter[None]
    bit = size // 2
    while bit:
        mine = (here // bit) % 2
        other = swap(held, axis, bit)
        first = jnp.where(mine == 0, held, other)
        second = jnp.where(mine == 0, other, held)
        held = jnp.stack([first, second], axis=1).reshape((-1,) + quarter.shape)
        bit //= 2
    return held.reshape((-1,) + quarter.shape[1:])


def polar(sigma_block):
    states = sigma_block.shape[0]
    mean_sq = jnp.sum(sigma_block * sigma_block) / float(states * states)
    iterate = sigma_block * (lax.rsqrt(states * mean_sq + 1e-06) / 2.2)

    def step(_, iterate):
        gram_matrix = jnp.einsum("ab,cb->ac", iterate, iterate, precision=precise)
        return 1.5 * iterate - 0.5 * dot(gram_matrix, iterate)

    return lax.fori_loop(0, POLAR, step, iterate) * math.sqrt(states)


def shards(wavefunction, left_env, right_env, shift_map, op_counts):
    sector_count = lax.axis_size("sector")
    group_size = lax.axis_size("ops")
    group_here = lax.axis_index("ops")
    states = wavefunction.shape[1]
    ops_here = left_env.shape[1]
    parts = sector_count * group_size
    piece = -(-states * states // (SUBLANES * LANES * parts))
    padded = piece * parts
    quarter = piece * sector_count

    whole_map = lax.all_gather(shift_map[0], "ops").reshape(parts)

    def fetch_from_quarter(own_quarter):
        pieces = own_quarter.reshape(sector_count, piece, SUBLANES, LANES)
        spread = lax.all_to_all(pieces, "sector", split_axis=0, concat_axis=0, tiled=True)
        picked = jnp.take(spread, whole_map, axis=0)
        landed = lax.all_to_all(picked, ("ops", "sector"), split_axis=0, concat_axis=0, tiled=True)
        return from_tiles(landed.reshape(padded, SUBLANES, LANES), states, states)

    psi_tiles = to_tiles(wavefunction[0], padded)
    psi_quarter = lax.dynamic_slice_in_dim(psi_tiles, group_here * quarter, quarter, 0)
    moved_block = fetch_from_quarter(psi_quarter)

    left, right = left_env[0], right_env[0]
    count = op_counts[0, 0]
    active = (jnp.arange(ops_here) < count).astype(jnp.float32)
    left_by_cols, left_by_rows, moved_block = lax.optimization_barrier(
        (stack_left(left, 2), stack_left(left, 1), moved_block)
    )
    left_psi = jnp.einsum(
        "wak,kc->wac", left_by_cols, stack_right(moved_block, 0), preferred_element_type=jnp.float32
    ) * active[:, None, None]
    partial_sigma = jnp.einsum("wac,wcd->ad", left_psi, right, precision=precise)

    sigma_quarter = sum_scatter(to_tiles(partial_sigma, padded), "ops")
    source_sigma = fetch_from_quarter(sigma_quarter)
    sigma_block = from_tiles(gather_whole(sigma_quarter, "ops"), states, states)

    whole_tensor = polar(sigma_block)
    column_width = states // group_size
    own_columns = lax.dynamic_slice_in_dim(whole_tensor, group_here * column_width, column_width, 1)
    half_rotated = jnp.einsum(
        "ka,wkc->wac", stack_right(whole_tensor, 0), left_by_rows, preferred_element_type=jnp.float32
    )
    source_tensor = polar(source_sigma)
    rotated = jnp.einsum("wac,cd->wad", half_rotated, source_tensor, precision=precise)
    return (own_columns[None], rotated[None])


def solution(mesh):
    return jax.shard_map(
        shards,
        mesh=mesh,
        in_specs=(
            P("sector", None, None),
            P("sector", "ops", None, None),
            P("sector", "ops", None, None),
            P("ops", None),
            P("ops", "sector"),
        ),
        out_specs=(P("sector", None, "ops"), P("sector", "ops", None, None)),
        check_vma=False,
    )
```
